32 devices in a mesh: rep: 2 (over x), dp: 16 (over y, z, core).
Axes of the slice: x: 2, y: 2, z: 4, core: 2. Of those that a mesh axis runs over, the one named last changes fastest.
Arguments:
- x: bfloat16 [32, 2048, 896], P(('rep', 'dp')), parts along dimension 0
- dy: bfloat16 [32, 2048, 896], P(('rep', 'dp')), parts along dimension 0
- w_gate: bfloat16 [2, 896, 2304], P(None, 'dp')
- w_up: bfloat16 [2, 896, 2304], P(None, 'dp')
- w_down: bfloat16 [2, 2304, 896], P(None, 'dp')
Outputs:
- output 1: bfloat16 [32, 2048, 896], P(('rep', 'dp')), parts along dimension 0
- output 2: bfloat16 [4, 896, 2304], P('rep', 'dp'), parts along dimension 0
- output 3: bfloat16 [4, 896, 2304], P('rep', 'dp'), parts along dimension 0
- output 4: bfloat16 [4, 2304, 896], P('rep', 'dp'), parts along dimension 0
There are 2 independent parts. The reference program is written for one: setup_inputs(seed, part) draws one part's arguments, and reference() takes and returns one part's arrays. A program takes and returns all parts, laid end to end along the dimension named above; an argument that names none is the same for every part.
All inputs are finite; a program needn't handle non-finite values.
Results may differ from the reference program's by a relative error of at most 0.018.
Values are sent between devices in bfloat16 or wider.
A program may use at most 2 GiB of HBM per device.

```python
import jax
import jax.numpy as jnp
from jax import lax

SEQUENCES = 16
TOKENS = 2048
D = 896
FF = 2304
LAYERS = 2
NAMES = ("w_gate", "w_up", "w_down")
SHAPES = {"w_gate": (LAYERS, D, FF), "w_up": (LAYERS, D, FF), "w_down": (LAYERS, FF, D)}


def bump(key, n, height):
    away = (jnp.arange(n, dtype=jnp.int32) - jax.random.randint(key, (), 0, n, jnp.int32)) % n
    return jnp.where(away < n // 8, height, 1.0)


def together(key, own, strength):
    shared = jax.random.normal(key, own.shape[1:], jnp.float32)
    return (own + strength * shared) * lax.rsqrt(1 + strength * strength)


def setup_inputs(seed: int = 0, part: int = 0) -> dict:
    kx, kdy, ka, kb, kz, kf, kh, kl, *kw = jax.random.split(jax.random.key(seed), 8 + len(NAMES))
    kx, kdy, ka, kb = (jax.random.fold_in(k, part) for k in (kx, kdy, ka, kb))
    shape = (SEQUENCES, TOKENS, D)
    much_x, much_dy = jax.random.uniform(kz, (2,), jnp.float32, 0.0, 1.0)
    layers = 2.0 ** jax.random.uniform(kl, (LAYERS, 1, 1), jnp.float32, -1.0, 1.0)
    x = together(ka, jax.random.normal(kx, shape, jnp.float32), much_x) * bump(kf, D, 4.0)
    dy = together(kb, jax.random.normal(kdy, shape, jnp.float32), much_dy)
    drawn = {"x": x.astype(jnp.bfloat16), "dy": (dy * (SEQUENCES * TOKENS) ** -0.5).astype(jnp.bfloat16)}
    for key, name in zip(kw, NAMES, strict=True):
        w = jax.random.normal(key, SHAPES[name], jnp.float32) * SHAPES[name][1] ** -0.5
        drawn[name] = (w * {"w_gate": 1.0, "w_up": bump(kh, FF, 4.0), "w_down": layers}[name]).astype(jnp.bfloat16)
    return drawn


def matmul(a, w):
    return jnp.dot(a, w, preferred_element_type=jnp.float32).astype(jnp.bfloat16)


def normed(h):
    wide = h.astype(jnp.float32)
    scale = lax.rsqrt(jnp.mean(wide**2, -1, keepdims=True) + 1e-6)
    return (wide * scale).astype(jnp.bfloat16)


def layer(h, w):
    a = normed(h)
    gate = jnp.dot(a, w["w_gate"], preferred_element_type=jnp.float32)
    up = jnp.dot(a, w["w_up"], preferred_element_type=jnp.float32)
    return h + matmul((jax.nn.silu(gate) * up).astype(jnp.bfloat16), w["w_down"])


def stack(weights, h):
    return lax.scan(lambda h, w: (layer(h, w), None), h, weights)[0]


def reference(x, dy, w_gate, w_up, w_down):
    weights = dict(zip(NAMES, (w_gate, w_up, w_down), strict=True))

    def take(so_far, sequence):
        h, by_y = sequence
        _, back = jax.vjp(stack, weights, h)
        by_weights, by_h = back(by_y)
        return jax.tree.map(lambda total, term: total + term.astype(jnp.float32), so_far, by_weights), by_h

    none_yet = {name: jnp.zeros(w.shape, jnp.float32) for name, w in weights.items()}
    by_weights, by_x = lax.scan(take, none_yet, (x, dy))
    return (by_x, *(by_weights[name].astype(jnp.bfloat16) for name in NAMES))
```

```python
import jax
import jax.numpy as jnp
from jax import lax
from jax.experimental import pallas as pl
from jax.experimental.pallas import tpu as pltpu
from jax.sharding import PartitionSpec as P


MESH = pl.DeviceIdType.MESH
Z = 4


def gather_kernel(gu_ref, d_ref, gu_out, d_out, s1s, s1r, s2s, s2r, s3s, s3r, s4s, s4r, loc):
    x, me = lax.axis_index("rep"), lax.axis_index("dp")
    y, z, c = me // 8, (me // 2) % 4, me % 2

    def at(yy, zz, cc):
        return (yy * Z + zz) * 2 + cc

    def zx(k):
        if k == 2:
            return (z + 2) % 4
        other = z + 1 - 2 * (z % 2)
        return other if k == 1 else 3 - z

    zs = [z, zx(1), zx(2), zx(3)]
    y_peer, c_peer, x_peer = (x, at(1 - y, z, c)), (x, at(y, z, 1 - c)), (1 - x, me)
    peers = [(x, at(y, zs[k], c)) for k in (1, 2, 3)] + [y_peer, c_peer, x_peer]
    barrier = pltpu.get_barrier_semaphore()
    for peer in peers:
        pl.semaphore_signal(barrier, inc=1, device_id=peer, device_id_type=MESH)
    pl.semaphore_wait(barrier, len(peers))

    pending = []

    def send(src, dst, ss, rs, peer):
        copy = pltpu.make_async_remote_copy(src, dst, ss, rs, device_id=peer, device_id_type=MESH)
        copy.start()
        pending.append(copy)
        return copy

    locals_ = []
    groups = [(0, True), (0, False), (1, True), (1, False)]
    first, second, third, fourth = {}, {}, {}, []

    def own(l, gu):
        return gu_ref.at[x, l] if gu else d_ref.at[l]

    def place(l, gu, b, m=None):
        return gu_out.at[x if m is None else m, l, b] if gu else d_out.at[l, b]

    for g, (l, gu) in enumerate(groups):
        for k in (1, 2, 3):
            first[g, k] = send(own(l, gu), place(l, gu, me), s1s.at[g, k - 1], s1r.at[g, k - 1], (x, at(y, zs[k], c)))
    fourth_count = [0] * 4

    def to_core(g, src, dst):
        n = fourth_count[g]
        fourth_count[g] += 1
        fourth.append(send(src, dst, s4s.at[g, n], s4r.at[g, n], c_peer))

    for g, (l, gu) in enumerate(groups):
        second[g, 0] = send(own(l, gu), place(l, gu, me), s2s.at[g, 0], s2r.at[g, 0], y_peer)
        for m in (0, 1) if gu else (0,):
            src = gu_ref.at[m, l] if gu else d_ref.at[l]
            dst = gu_out.at[m, l, me] if gu else d_out.at[l, me]
            to_core(g, src, dst)
            copy = pltpu.make_async_copy(src, dst, loc.at[2 * g + m])
            copy.start()
            locals_.append(copy)

    def arrive_first(g, k):
        l, gu = groups[g]
        first[g, k].wait_recv()
        b = at(y, zs[k], c)
        ref = place(l, gu, b)
        second[g, k] = send(ref, ref, s2s.at[g, k], s2r.at[g, k], y_peer)
        if gu:
            third[g, k - 1] = send(ref, ref, s3s.at[g // 2, k - 1], s3r.at[g // 2, k - 1], x_peer)
        to_core(g, ref, ref)

    def arrive_second(g, k):
        l, gu = groups[g]
        second[g, k].wait_recv()
        ref = place(l, gu, at(1 - y, zs[k], c))
        if gu:
            third[g, 3 + k] = send(ref, ref, s3s.at[g // 2, 3 + k], s3r.at[g // 2, 3 + k], x_peer)
        to_core(g, ref, ref)

    def arrive_third(g, j):
        l, gu = groups[g]
        third[g, j].wait_recv()
        b = at(y, zs[j + 1], c) if j < 3 else at(1 - y, zs[j - 3], c)
        ref = place(l, gu, b, 1 - x)
        to_core(g, ref, ref)

    events = []
    for g, (l, gu) in enumerate(groups):
        events += [(4 * g + k + 1.0, 0, arrive_first, g, k) for k in (1, 2, 3)]
        events += [(4 * g + k + 2.5, 1, arrive_second, g, k) for k in range(4)]
        if gu:
            events += [(7 * (g // 2) + j + 3.7, 2, arrive_third, g, j) for j in range(7)]
    for _, _, what, g, k in sorted(events, key=lambda e: e[:2]):
        what(g, k)
    for copy in fourth:
        copy.wait_recv()
    for copy in pending:
        copy.wait_send()
    for copy in locals_:
        copy.wait()


def gather(w_gate, w_up, w_down):
    gu = jnp.stack([w_gate, w_up])
    any_ = pl.BlockSpec(memory_space=pl.ANY)
    dma = pltpu.SemaphoreType.DMA
    _, layers, rows, ff = gu.shape
    _, rows_d, d = w_down.shape
    n = 16
    gu, down = pl.pallas_call(
        gather_kernel,
        out_shape=(
            jax.ShapeDtypeStruct((2, layers, n, rows, ff), gu.dtype),
            jax.ShapeDtypeStruct((layers, n, rows_d, d), gu.dtype),
        ),
        in_specs=[any_] * 2,
        out_specs=(any_, any_),
        scratch_shapes=[
            dma((4, 3)), dma((4, 3)), dma((4, 4)), dma((4, 4)), dma((2, 7)), dma((2, 7)),
            dma((4, 16)), dma((4, 16)), dma((8,)),
        ],
        compiler_params=pltpu.CompilerParams(collective_id=0, has_side_effects=True),
    )(gu, w_down)
    gu = gu.reshape(2, layers, n * rows, ff)
    down = down.reshape(layers, n * rows_d, d)
    return [(gu[0, l], gu[1, l], down[l]) for l in range(layers)]


def dot(a, b, ca, cb):
    return lax.dot_general(a, b, (((ca,), (cb,)), ((), ())), preferred_element_type=jnp.float32)


def pairs(of):
    return [((y * Z + z) * 2 + c, of(y, z, c)) for y in range(2) for z in range(Z) for c in range(2)]


def scatter_sum(term):
    me = lax.axis_index("dp")
    y, z, c = me // 8, (me // 2) % 4, me % 2
    term = term.reshape(2, Z, 2, -1, term.shape[-1])

    def pick(t, i, axis):
        return lax.dynamic_index_in_dim(t, i, axis, keepdims=False)

    def swap(t, of):
        t = t.astype(jnp.bfloat16)
        t = lax.ppermute(t, "dp", pairs(of))
        return t.astype(jnp.float32)

    got = swap(pick(term, 1 - c, 2), lambda y, z, c: (y * Z + z) * 2 + 1 - c)
    term = pick(term, c, 2) + got
    got = swap(pick(term, 1 - y, 0), lambda y, z, c: ((1 - y) * Z + z) * 2 + c)
    term = pick(term, y, 0) + got
    total = pick(term, z, 0)
    for k in (1, 2, 3):
        total += swap(pick(term, z ^ k, 0), lambda y, z, c: (y * Z + (z ^ k)) * 2 + c)
    return total.astype(jnp.bfloat16)


def solution(mesh):
    def step(*args):
        return work(*args)

    def work(x, dy, w_gate, w_up, w_down):
        x, dy = x[0], dy[0]
        bf16, f32 = jnp.bfloat16, jnp.float32
        weights = gather(w_gate, w_up, w_down)
        h, saved = x, []
        for wg, wu, wd in weights:
            wide = h.astype(f32)
            scale = lax.rsqrt(jnp.mean(wide**2, -1, keepdims=True) + 1e-6)
            a = (wide * scale).astype(bf16)
            gate, up = dot(a, wg, 1, 0), dot(a, wu, 1, 0)
            p = (jax.nn.silu(gate) * up).astype(bf16)
            saved.append((h, scale, a, gate, up, p))
            if len(saved) < len(weights):
                h = h + dot(p, wd, 1, 0).astype(bf16)
        outs = []
        for l in reversed(range(len(weights))):
            wg, wu, wd = weights[l]
            h, scale, a, gate, up, p = saved[l]
            by_d = scatter_sum(dot(p, dy, 0, 0))
            dp = dot(dy, wd, 1, 1).astype(bf16).astype(f32)
            s = jax.nn.sigmoid(gate)
            silu = gate * s
            dup = (dp * silu).astype(bf16)
            dgate = (dp * up * (s * (1 + gate * (1 - s)))).astype(bf16)
            by_g = scatter_sum(dot(a, dgate, 0, 0))
            by_u = scatter_sum(dot(a, dup, 0, 0))
            da = (dot(dgate, wg, 1, 1).astype(bf16) + dot(dup, wu, 1, 1).astype(bf16)).astype(f32)
            wide = h.astype(f32)
            dh = scale * (da - wide * (scale**2 * jnp.mean(da * wide, -1, keepdims=True)))
            dy = dy + dh.astype(bf16)
            outs.append((by_g, by_u, by_d))
        outs = outs[::-1]
        return (dy[None], *(jnp.stack([o[i] for o in outs]) for i in range(3)))

    rows = P(("rep", "dp"), None, None)
    w = P(None, "dp", None)
    g = P("rep", "dp", None)
    step = jax.shard_map(step, mesh=mesh, in_specs=(rows, rows, w, w, w), out_specs=(rows, g, g, g), check_vma=False)
    return step
```

```python
import jax
import jax.numpy as jnp
from jax import lax
from jax.experimental import pallas as pl
from jax.experimental.pallas import tpu as pltpu
from jax.sharding import PartitionSpec as P


MESH = pl.DeviceIdType.MESH
Z = 4


def gather_kernel(gu_ref, d_ref, gu_out, d_out, s1s, s1r, s2s, s2r, s3s, s3r, s4s, s4r, loc):
    x, me = lax.axis_index("rep"), lax.axis_index("dp")
    y, z, c = me // 8, (me // 2) % 4, me % 2

    def at(yy, zz, cc):
        return (yy * Z + zz) * 2 + cc

    def zx(k):
        if k == 2:
            return (z + 2) % 4
        other = z + 1 - 2 * (z % 2)
        return other if k == 1 else 3 - z

    zs = [z, zx(1), zx(2), zx(3)]
    y_peer, c_peer, x_peer = (x, at(1 - y, z, c)), (x, at(y, z, 1 - c)), (1 - x, me)
    peers = [(x, at(y, zs[k], c)) for k in (1, 2, 3)] + [y_peer, c_peer, x_peer]
    barrier = pltpu.get_barrier_semaphore()
    for peer in peers:
        pl.semaphore_signal(barrier, inc=1, device_id=peer, device_id_type=MESH)
    pl.semaphore_wait(barrier, len(peers))

    pending = []

    def send(src, dst, ss, rs, peer):
        copy = pltpu.make_async_remote_copy(src, dst, ss, rs, device_id=peer, device_id_type=MESH)
        copy.start()
        pending.append(copy)
        return copy

    locals_ = []
    groups = [(0, True), (0, False), (1, True), (1, False)]
    first, second, third, fourth = {}, {}, {}, []

    def own(l, gu):
        return gu_ref.at[x, l] if gu else d_ref.at[l]

    def place(l, gu, b, m=None):
        return gu_out.at[x if m is None else m, l, b] if gu else d_out.at[l, b]

    for g, (l, gu) in enumerate(groups):
        for k in (1, 2, 3):
            first[g, k] = send(own(l, gu), place(l, gu, me), s1s.at[g, k - 1], s1r.at[g, k - 1], (x, at(y, zs[k], c)))
    fourth_count = [0] * 4

    def to_core(g, src, dst):
        n = fourth_count[g]
        fourth_count[g] += 1
        fourth.append(send(src, dst, s4s.at[g, n], s4r.at[g, n], c_peer))

    for g, (l, gu) in enumerate(groups):
        second[g, 0] = send(own(l, gu), place(l, gu, me), s2s.at[g, 0], s2r.at[g, 0], y_peer)
        for m in (0, 1) if gu else (0,):
            src = gu_ref.at[m, l] if gu else d_ref.at[l]
            dst = gu_out.at[m, l, me] if gu else d_out.at[l, me]
            to_core(g, src, dst)
            copy = pltpu.make_async_copy(src, dst, loc.at[2 * g + m])
            copy.start()
            locals_.append(copy)

    def arrive_first(g, k):
        l, gu = groups[g]
        first[g, k].wait_recv()
        b = at(y, zs[k], c)
        ref = place(l, gu, b)
        second[g, k] = send(ref, ref, s2s.at[g, k], s2r.at[g, k], y_peer)
        if gu:
            third[g, k - 1] = send(ref, ref, s3s.at[g // 2, k - 1], s3r.at[g // 2, k - 1], x_peer)
        to_core(g, ref, ref)

    def arrive_second(g, k):
        l, gu = groups[g]
        second[g, k].wait_recv()
        ref = place(l, gu, at(1 - y, zs[k], c))
        if gu:
            third[g, 3 + k] = send(ref, ref, s3s.at[g // 2, 3 + k], s3r.at[g // 2, 3 + k], x_peer)
        to_core(g, ref, ref)

    def arrive_third(g, j):
        l, gu = groups[g]
        third[g, j].wait_recv()
        b = at(y, zs[j + 1], c) if j < 3 else at(1 - y, zs[j - 3], c)
        ref = place(l, gu, b, 1 - x)
        to_core(g, ref, ref)

    events = []
    for g, (l, gu) in enumerate(groups):
        events += [(4 * g + k + 1.0, 0, arrive_first, g, k) for k in (1, 2, 3)]
        events += [(4 * g + k + 2.5, 1, arrive_second, g, k) for k in range(4)]
        if gu:
            events += [(7 * (g // 2) + j + 3.7, 2, arrive_third, g, j) for j in range(7)]
    for _, _, what, g, k in sorted(events, key=lambda e: e[:2]):
        what(g, k)
    for copy in fourth:
        copy.wait_recv()
    for copy in pending:
        copy.wait_send()
    for copy in locals_:
        copy.wait()


def gather(w_gate, w_up, w_down):
    gu = jnp.stack([w_gate, w_up])
    any_ = pl.BlockSpec(memory_space=pl.ANY)
    dma = pltpu.SemaphoreType.DMA
    _, layers, rows, ff = gu.shape
    _, rows_d, d = w_down.shape
    n = 16
    gu, down = pl.pallas_call(
        gather_kernel,
        out_shape=(
            jax.ShapeDtypeStruct((2, layers, n, rows, ff), gu.dtype),
            jax.ShapeDtypeStruct((layers, n, rows_d, d), gu.dtype),
        ),
        in_specs=[any_] * 2,
        out_specs=(any_, any_),
        scratch_shapes=[
            dma((4, 3)), dma((4, 3)), dma((4, 4)), dma((4, 4)), dma((2, 7)), dma((2, 7)),
            dma((4, 16)), dma((4, 16)), dma((8,)),
        ],
        compiler_params=pltpu.CompilerParams(collective_id=0, has_side_effects=True),
    )(gu, w_down)
    return gu.reshape(2, layers, n * rows, ff), down.reshape(layers, n * rows_d, d)


TILE, CHUNK = 512, 768


def mm(a, b, cb=0):
    return lax.dot_general(a, b, (((1,), (cb,)), ((), ())), preferred_element_type=jnp.float32)


def normed(h):
    wide = h.astype(jnp.float32)
    scale = lax.rsqrt(jnp.mean(wide**2, -1, keepdims=True) + 1e-6)
    return wide, scale


def chunks(ff):
    return [pl.ds(i, CHUNK) for i in range(0, ff, CHUNK)]


def forward_kernel(h_ref, wg, wu, wd, next_ref, a_ref, p_ref, gate_ref, up_ref):
    wide, scale = normed(h_ref[...])
    a = (wide * scale).astype(jnp.bfloat16)
    a_ref[...] = a
    total = None
    for c in chunks(wg.shape[-1]):
        gate, up = mm(a, wg[:, c]), mm(a, wu[:, c])
        gate_ref[:, c], up_ref[:, c] = gate, up
        p = (gate * jax.nn.sigmoid(gate) * up).astype(jnp.bfloat16)
        p_ref[:, c] = p
        part = mm(p, wd[c, :])
        total = part if total is None else total + part
    next_ref[...] = (wide + total.astype(jnp.bfloat16).astype(jnp.float32)).astype(jnp.bfloat16)


def through_gate(gate, up, dp):
    dp = dp.astype(jnp.bfloat16).astype(jnp.float32)
    s = jax.nn.sigmoid(gate)
    silu = gate * s
    dgate = (dp * up * (s * (1 + gate * (1 - s)))).astype(jnp.bfloat16)
    return silu, dgate, (dp * silu).astype(jnp.bfloat16)


def through_norm(wide, scale, dy, da_gate, da_up):
    bf16, f32 = jnp.bfloat16, jnp.float32
    da = (da_gate.astype(bf16).astype(f32) + da_up.astype(bf16).astype(f32)).astype(bf16).astype(f32)
    dh = scale * (da - wide * (scale**2 * jnp.mean(da * wide, -1, keepdims=True)))
    return (dy.astype(f32) + dh.astype(bf16).astype(f32)).astype(bf16)


def last_kernel(h_ref, dy_ref, wg, wu, wd, dh_ref, a_ref, p_ref, dgate_ref, dup_ref):
    wide, scale = normed(h_ref[...])
    a = (wide * scale).astype(jnp.bfloat16)
    a_ref[...] = a
    dy = dy_ref[...]
    da_gate = da_up = None
    for c in chunks(wg.shape[-1]):
        gate, up = mm(a, wg[:, c]), mm(a, wu[:, c])
        silu, dgate, dup = through_gate(gate, up, mm(dy, wd[c, :], 1))
        p_ref[:, c] = (silu * up).astype(jnp.bfloat16)
        dgate_ref[:, c], dup_ref[:, c] = dgate, dup
        g, u = mm(dgate, wg[:, c], 1), mm(dup, wu[:, c], 1)
        da_gate, da_up = (g, u) if da_gate is None else (da_gate + g, da_up + u)
    dh_ref[...] = through_norm(wide, scale, dy, da_gate, da_up)


def gate_kernel(dy_ref, gate_ref, up_ref, wd, dgate_ref, dup_ref):
    dy = dy_ref[...]
    for c in chunks(gate_ref.shape[-1]):
        _, dgate_ref[:, c], dup_ref[:, c] = through_gate(gate_ref[:, c], up_ref[:, c], mm(dy, wd[c, :], 1))


def input_kernel(h_ref, dy_ref, dgate_ref, dup_ref, wg, wu, dh_ref):
    wide, scale = normed(h_ref[...])
    da_gate, da_up = mm(dgate_ref[...], wg[...], 1), mm(dup_ref[...], wu[...], 1)
    dh_ref[...] = through_norm(wide, scale, dy_ref[...], da_gate, da_up)


def call(kernel, tokens, weights, outs, matmuls):
    t = tokens[0].shape[0]
    d, ff = 896, 2304
    specs = [pl.BlockSpec((TILE, v.shape[1]), lambda i: (i, 0)) for v in tokens]
    for w, at in weights:
        specs.append(
            pl.BlockSpec((None,) * len(at) + w.shape[-2:], lambda i, at=at: (*at, 0, 0), pipeline_mode=pl.Buffered(1))
        )
    return pl.pallas_call(
        kernel,
        grid=(t // TILE,),
        in_specs=specs,
        out_specs=[pl.BlockSpec((TILE, n), lambda i: (i, 0)) for n, _ in outs],
        out_shape=[jax.ShapeDtypeStruct((t, n), dtype) for n, dtype in outs],
        compiler_params=pltpu.CompilerParams(vmem_limit_bytes=60 * 2**20, dimension_semantics=("arbitrary",)),
        cost_estimate=pl.CostEstimate(flops=2 * t * d * ff * matmuls, bytes_accessed=30 * 2**20, transcendentals=t * ff),
    )(*tokens, *(w for w, _ in weights))


def dot(a, b, ca, cb):
    return lax.dot_general(a, b, (((ca,), (cb,)), ((), ())), preferred_element_type=jnp.float32)


def pairs(of):
    return [((y * Z + z) * 2 + c, of(y, z, c)) for y in range(2) for z in range(Z) for c in range(2)]


def scatter_sum(term):
    me = lax.axis_index("dp")
    y, z, c = me // 8, (me // 2) % 4, me % 2
    term = lax.optimization_barrier(term).reshape(2, Z, 2, -1, term.shape[-1])

    def pick(t, i, axis):
        return lax.dynamic_index_in_dim(t, i, axis, keepdims=False)

    def swap(t, of):
        t = t.astype(jnp.bfloat16)
        t = lax.ppermute(t, "dp", pairs(of))
        return t.astype(jnp.float32)

    got = swap(pick(term, 1 - c, 2), lambda y, z, c: (y * Z + z) * 2 + 1 - c)
    term = pick(term, c, 2) + got
    got = swap(pick(term, 1 - y, 0), lambda y, z, c: ((1 - y) * Z + z) * 2 + c)
    term = pick(term, y, 0) + got
    total = pick(term, z, 0)
    for k in (1, 2, 3):
        total += swap(pick(term, z ^ k, 0), lambda y, z, c: (y * Z + (z ^ k)) * 2 + c)
    return total.astype(jnp.bfloat16)


def solution(mesh):
    def step(*args):
        return work(*args)

    def work(x, dy, w_gate, w_up, w_down):
        x, dy = x[0], dy[0]
        bf16, f32 = jnp.bfloat16, jnp.float32
        gu, down = gather(w_gate, w_up, w_down)
        d, ff = x.shape[1], gu.shape[-1]
        wg, wu, wd = [[(gu, (0, l)) for l in (0, 1)], [(gu, (1, l)) for l in (0, 1)], [(down, (l,)) for l in (0, 1)]]
        h, a0, p0, gate, up = call(
            forward_kernel, (x,), (wg[0], wu[0], wd[0]), [(d, bf16), (d, bf16), (ff, bf16), (ff, f32), (ff, f32)], 3
        )
        dy0, a1, p1, dgate1, dup1 = call(
            last_kernel, (h, dy), (wg[1], wu[1], wd[1]), [(d, bf16), (d, bf16), (ff, bf16), (ff, bf16), (ff, bf16)], 5
        )
        d1 = scatter_sum(dot(p1, dy, 0, 0))
        g1 = scatter_sum(dot(a1, dgate1, 0, 0))
        u1 = scatter_sum(dot(a1, dup1, 0, 0))
        d0 = scatter_sum(dot(p0, dy0, 0, 0))
        dgate0, dup0 = call(gate_kernel, (dy0, gate, up), (wd[0],), [(ff, bf16), (ff, bf16)], 1)
        g0 = scatter_sum(dot(a0, dgate0, 0, 0))
        u0 = scatter_sum(dot(a0, dup0, 0, 0))
        (dx,) = call(input_kernel, (x, dy0, dgate0, dup0), (wg[0], wu[0]), [(d, bf16)], 2)
        return dx[None], jnp.stack([g0, g1]), jnp.stack([u0, u1]), jnp.stack([d0, d1])

    rows = P(("rep", "dp"), None, None)
    w = P(None, "dp", None)
    g = P("rep", "dp", None)
    step = jax.shard_map(step, mesh=mesh, in_specs=(rows, rows, w, w, w), out_specs=(rows, g, g, g), check_vma=False)
    return step
```

```python
import jax
import jax.numpy as jnp
from jax import lax
from jax.experimental import pallas as pl
from jax.experimental.pallas import tpu as pltpu
from jax.sharding import PartitionSpec as P


MESH = pl.DeviceIdType.MESH
Z = 4


TILE, CHUNK = 512, 768
FIRST_TILE = 256


def mm(a, b, cb=0):
    return lax.dot_general(a, b, (((1,), (cb,)), ((), ())), preferred_element_type=jnp.float32)


def normed(h):
    wide = h.astype(jnp.float32)
    scale = lax.rsqrt(jnp.mean(wide**2, -1, keepdims=True) + 1e-6)
    return wide, scale


def chunks(ff):
    return [pl.ds(i, CHUNK) for i in range(0, ff, CHUNK)]


def forward_kernel(h_ref, wg, wu, wd, next_ref, a_ref, p_ref, gate_ref, up_ref):
    wide, scale = normed(h_ref[...])
    a = (wide * scale).astype(jnp.bfloat16)
    a_ref[...] = a
    total = None
    for c in chunks(wg.shape[-1]):
        gate, up = mm(a, wg[:, c]), mm(a, wu[:, c])
        gate_ref[:, c], up_ref[:, c] = gate, up
        p = (gate * jax.nn.sigmoid(gate) * up).astype(jnp.bfloat16)
        p_ref[:, c] = p
        part = mm(p, wd[c, :])
        total = part if total is None else total + part
    next_ref[...] = (wide + total.astype(jnp.bfloat16).astype(jnp.float32)).astype(jnp.bfloat16)


def gather_kernel(
    h_ref, gu_ref, d_ref, gu_out, d_out, next_ref, a_ref, p_ref, gate_ref, up_ref,
    wg, wu, wd, s1s, s1r, s2s, s2r, s3s, s3r, s4s, s4r, loc, load,
):
    step, steps = pl.program_id(0), pl.num_programs(0)
    x, me = lax.axis_index("rep"), lax.axis_index("dp")
    y, z, c = me // 8, (me // 2) % 4, me % 2
    rows, rows_d = gu_ref.shape[2], d_ref.shape[1]

    def at(yy, zz, cc):
        return (yy * Z + zz) * 2 + cc

    other = z + 1 - 2 * (z % 2)
    zs = [z, other, (z + 2) % 4, 3 - z]
    y_peer, c_peer, x_peer = (x, at(1 - y, z, c)), (x, at(y, z, 1 - c)), (1 - x, me)
    peers = [(x, at(y, zs[k], c)) for k in (1, 2, 3)] + [y_peer, c_peer, x_peer]

    groups = [(0, True), (0, False), (1, True), (1, False)]
    first, second, third = {}, {}, {}
    fourth = [[] for _ in groups]
    everything, locals_ = [], []

    def remote(src, dst, ss, rs, peer):
        copy = pltpu.make_async_remote_copy(src, dst, ss, rs, device_id=peer, device_id_type=MESH)
        everything.append(copy)
        return copy

    def own(l, gu, m):
        return gu_ref.at[m, l] if gu else d_ref.at[l]

    def place(l, gu, b, m):
        if gu:
            return gu_out.at[m, l, pl.ds(pl.multiple_of(b * rows, 8), rows)]
        return d_out.at[l, pl.ds(pl.multiple_of(b * rows_d, 16), rows_d)]

    def to_core(g, src, dst):
        n = len(fourth[g])
        copy = remote(src, dst, s4s.at[g, n], s4r.at[g, n], c_peer)
        fourth[g].append(copy)
        return copy

    begin, events = [], []
    for g, (l, gu) in enumerate(groups):
        for k in (1, 2, 3):
            peer = (x, at(y, zs[k], c))
            first[g, k] = remote(own(l, gu, x), place(l, gu, me, x), s1s.at[g, k - 1], s1r.at[g, k - 1], peer)
            begin.append(first[g, k])
    for g, (l, gu) in enumerate(groups):
        second[g, 0] = remote(own(l, gu, x), place(l, gu, me, x), s2s.at[g, 0], s2r.at[g, 0], y_peer)
        begin.append(second[g, 0])
        for m in (0, 1) if gu else (0,):
            src, dst = own(l, gu, m), place(l, gu, me, m)
            begin.append(to_core(g, src, dst))
            locals_.append(pltpu.make_async_copy(src, dst, loc.at[2 * g + m]))
            begin.append(locals_[-1])
    for g, (l, gu) in enumerate(groups):
        for k in (1, 2, 3):
            ref = place(l, gu, at(y, zs[k], c), x)
            second[g, k] = remote(ref, ref, s2s.at[g, k], s2r.at[g, k], y_peer)
            starts = [second[g, k]]
            if gu:
                third[g, k - 1] = remote(ref, ref, s3s.at[g // 2, k - 1], s3r.at[g // 2, k - 1], x_peer)
                starts.append(third[g, k - 1])
            events.append((4 * g + k + 1.0, l, first[g, k], starts + [to_core(g, ref, ref)]))
        for k in range(4):
            ref = place(l, gu, at(1 - y, zs[k], c), x)
            starts = []
            if gu:
                third[g, 3 + k] = remote(ref, ref, s3s.at[g // 2, 3 + k], s3r.at[g // 2, 3 + k], x_peer)
                starts.append(third[g, 3 + k])
            events.append((4 * g + k + 2.5, l, second[g, k], starts + [to_core(g, ref, ref)]))
        if gu:
            for j in range(7):
                b = at(y, zs[j + 1], c) if j < 3 else at(1 - y, zs[j - 3], c)
                ref = place(l, gu, b, 1 - x)
                events.append((7 * (g // 2) + j + 3.7, l, third[g, j], [to_core(g, ref, ref)]))
    events.sort(key=lambda e: (e[1], e[0]))

    def run(some):
        for _, _, arrival, starts in some:
            arrival.wait_recv()
            for copy in starts:
                copy.start()

    early = [e for e in events if e[1] == 0]
    late = [e for e in events if e[1] == 1]
    in_vmem = [
        pltpu.make_async_copy(src, dst, load.at[n])
        for n, (src, dst) in enumerate([(gu_out.at[0, 0], wg), (gu_out.at[1, 0], wu), (d_out.at[0], wd)])
    ]

    @pl.when(step == 0)
    def _():
        barrier = pltpu.get_barrier_semaphore()
        for peer in peers:
            pl.semaphore_signal(barrier, inc=1, device_id=peer, device_id_type=MESH)
        pl.semaphore_wait(barrier, len(peers))
        for copy in begin:
            copy.start()
        run(early)
        for copy in fourth[0] + fourth[1]:
            copy.wait_recv()
        for copy in locals_:
            copy.wait()
        for copy in in_vmem:
            copy.start()
        for copy in in_vmem:
            copy.wait()

    done = 0
    for n in range(1, TOKENS // FIRST_TILE):
        some = [e for e in late[done:] if e[0] <= 10.5 + 0.9 * n]
        done += len(some)
        if some:
            @pl.when(step == n)
            def _(some=some):
                run(some)

    forward_kernel(h_ref, wg, wu, wd, next_ref, a_ref, p_ref, gate_ref, up_ref)

    @pl.when(step == steps - 1)
    def _():
        run(late[done:])
        for copy in fourth[2] + fourth[3]:
            copy.wait_recv()
        for copy in everything:
            copy.wait_send()


TOKENS = 2048


def gather(h, w_gate, w_up, w_down):
    gu = jnp.stack([w_gate, w_up])
    any_ = pl.BlockSpec(memory_space=pl.ANY)
    dma = pltpu.SemaphoreType.DMA
    _, layers, rows, ff = gu.shape
    _, rows_d, d = w_down.shape
    n, t, bf16, f32 = 16, h.shape[0], gu.dtype, jnp.float32
    outs = [(d, bf16), (d, bf16), (ff, bf16), (ff, f32), (ff, f32)]

    def tile(width):
        return pl.BlockSpec((FIRST_TILE, width), lambda i: (i, 0))

    return pl.pallas_call(
        gather_kernel,
        grid=(t // FIRST_TILE,),
        out_shape=[
            jax.ShapeDtypeStruct((2, layers, n * rows, ff), bf16),
            jax.ShapeDtypeStruct((layers, n * rows_d, d), bf16),
        ] + [jax.ShapeDtypeStruct((t, width), dtype) for width, dtype in outs],
        in_specs=[tile(d), any_, any_],
        out_specs=[any_, any_] + [tile(width) for width, _ in outs],
        scratch_shapes=[
            pltpu.VMEM((n * rows, ff), bf16), pltpu.VMEM((n * rows, ff), bf16), pltpu.VMEM((n * rows_d, d), bf16),
            dma((4, 3)), dma((4, 3)), dma((4, 4)), dma((4, 4)), dma((2, 7)), dma((2, 7)),
            dma((4, 16)), dma((4, 16)), dma((8,)), dma((3,)),
        ],
        compiler_params=pltpu.CompilerParams(
            collective_id=0, has_side_effects=True, vmem_limit_bytes=60 * 2**20, dimension_semantics=("arbitrary",)
        ),
    )(h, gu, w_down)


def through_gate(gate, up, dp):
    dp = dp.astype(jnp.bfloat16).astype(jnp.float32)
    s = jax.nn.sigmoid(gate)
    silu = gate * s
    dgate = (dp * up * (s * (1 + gate * (1 - s)))).astype(jnp.bfloat16)
    return silu, dgate, (dp * silu).astype(jnp.bfloat16)


def through_norm(wide, scale, dy, da_gate, da_up):
    bf16, f32 = jnp.bfloat16, jnp.float32
    da = (da_gate.astype(bf16).astype(f32) + da_up.astype(bf16).astype(f32)).astype(bf16).astype(f32)
    dh = scale * (da - wide * (scale**2 * jnp.mean(da * wide, -1, keepdims=True)))
    return (dy.astype(f32) + dh.astype(bf16).astype(f32)).astype(bf16)


def last_kernel(h_ref, dy_ref, wg, wu, wd, dh_ref, a_ref, p_ref, dgate_ref, dup_ref):
    wide, scale = normed(h_ref[...])
    a = (wide * scale).astype(jnp.bfloat16)
    a_ref[...] = a
    dy = dy_ref[...]
    da_gate = da_up = None
    for c in chunks(wg.shape[-1]):
        gate, up = mm(a, wg[:, c]), mm(a, wu[:, c])
        silu, dgate, dup = through_gate(gate, up, mm(dy, wd[c, :], 1))
        p_ref[:, c] = (silu * up).astype(jnp.bfloat16)
        dgate_ref[:, c], dup_ref[:, c] = dgate, dup
        g, u = mm(dgate, wg[:, c], 1), mm(dup, wu[:, c], 1)
        da_gate, da_up = (g, u) if da_gate is None else (da_gate + g, da_up + u)
    dh_ref[...] = through_norm(wide, scale, dy, da_gate, da_up)


def gate_kernel(dy_ref, gate_ref, up_ref, wd, dgate_ref, dup_ref):
    dy = dy_ref[...]
    for c in chunks(gate_ref.shape[-1]):
        _, dgate_ref[:, c], dup_ref[:, c] = through_gate(gate_ref[:, c], up_ref[:, c], mm(dy, wd[c, :], 1))


def input_kernel(h_ref, dy_ref, dgate_ref, dup_ref, wg, wu, dh_ref):
    wide, scale = normed(h_ref[...])
    da_gate, da_up = mm(dgate_ref[...], wg[...], 1), mm(dup_ref[...], wu[...], 1)
    dh_ref[...] = through_norm(wide, scale, dy_ref[...], da_gate, da_up)


def call(kernel, tokens, weights, outs, matmuls, t=None, part=0):
    t = t or tokens[0].shape[0]
    d, ff, skip = 896, 2304, part * t // TILE
    specs = [pl.BlockSpec((TILE, v.shape[1]), lambda i: (i + skip, 0)) for v in tokens]
    for w, at in weights:
        specs.append(
            pl.BlockSpec((None,) * len(at) + w.shape[-2:], lambda i, at=at: (*at, 0, 0), pipeline_mode=pl.Buffered(1))
        )
    return pl.pallas_call(
        kernel,
        grid=(t // TILE,),
        in_specs=specs,
        out_specs=[pl.BlockSpec((TILE, n), lambda i: (i, 0)) for n, _ in outs],
        out_shape=[jax.ShapeDtypeStruct((t, n), dtype) for n, dtype in outs],
        compiler_params=pltpu.CompilerParams(vmem_limit_bytes=60 * 2**20, dimension_semantics=("arbitrary",)),
        cost_estimate=pl.CostEstimate(flops=2 * t * d * ff * matmuls, bytes_accessed=30 * 2**20, transcendentals=t * ff),
    )(*tokens, *(w for w, _ in weights))


def dot(a, b, ca, cb):
    return lax.dot_general(a, b, (((ca,), (cb,)), ((), ())), preferred_element_type=jnp.float32)


def pairs(of):
    return [((y * Z + z) * 2 + c, of(y, z, c)) for y in range(2) for z in range(Z) for c in range(2)]


def scatter_sum(term):
    me = lax.axis_index("dp")
    y, z, c = me // 8, (me // 2) % 4, me % 2
    term = lax.optimization_barrier(term).reshape(2, Z, 2, -1, term.shape[-1])

    def pick(t, i, axis):
        return lax.dynamic_index_in_dim(t, i, axis, keepdims=False)

    def swap(t, of):
        t = t.astype(jnp.bfloat16)
        t = lax.ppermute(t, "dp", pairs(of))
        return t.astype(jnp.float32)

    got = swap(pick(term, 1 - c, 2), lambda y, z, c: (y * Z + z) * 2 + 1 - c)
    term = pick(term, c, 2) + got
    got = swap(pick(term, 1 - y, 0), lambda y, z, c: ((1 - y) * Z + z) * 2 + c)
    term = pick(term, y, 0) + got
    total = pick(term, z, 0)
    for k in (1, 2, 3):
        total += swap(pick(term, z ^ k, 0), lambda y, z, c: (y * Z + (z ^ k)) * 2 + c)
    return total.astype(jnp.bfloat16)


def solution(mesh):
    def step(*args):
        return work(*args)

    def work(x, dy, w_gate, w_up, w_down):
        x, dy = x[0], dy[0]
        bf16 = jnp.bfloat16
        gu, down, h, a0, p0, gate, up = gather(x, w_gate, w_up, w_down)
        d, ff = x.shape[1], gu.shape[-1]
        wg, wu, wd = [[(gu, (0, l)) for l in (0, 1)], [(gu, (1, l)) for l in (0, 1)], [(down, (l,)) for l in (0, 1)]]
        dy0, a1, p1, dgate1, dup1 = call(
            last_kernel, (h, dy), (wg[1], wu[1], wd[1]), [(d, bf16), (d, bf16), (ff, bf16), (ff, bf16), (ff, bf16)], 5
        )
        d1 = scatter_sum(dot(p1, dy, 0, 0))
        g1 = scatter_sum(dot(a1, dgate1, 0, 0))
        u1 = scatter_sum(dot(a1, dup1, 0, 0))
        d0 = scatter_sum(dot(p0, dy0, 0, 0))
        dgate0, dup0 = call(gate_kernel, (dy0, gate, up), (wd[0],), [(ff, bf16), (ff, bf16)], 1)
        g0 = scatter_sum(dot(a0, dgate0, 0, 0))
        u0 = scatter_sum(dot(a0, dup0, 0, 0))
        half = x.shape[0] // 2
        dx = jnp.concatenate([
            call(input_kernel, (x, dy0, dgate0, dup0), (wg[0], wu[0]), [(d, bf16)], 1, half, n)[0]
            for n in (0, 1)
        ])
        return dx[None], jnp.stack([g0, g1]), jnp.stack([u0, u1]), jnp.stack([d0, d1])

    rows = P(("rep", "dp"), None, None)
    w = P(None, "dp", None)
    g = P("rep", "dp", None)
    step = jax.shard_map(step, mesh=mesh, in_specs=(rows, rows, w, w, w), out_specs=(rows, g, g, g), check_vma=False)
    return step
```

```python
import jax
import jax.numpy as jnp
from jax import lax
from jax.experimental import pallas as pl
from jax.experimental.pallas import tpu as pltpu
from jax.sharding import PartitionSpec as P


MESH = pl.DeviceIdType.MESH
Z = 4


TILE, CHUNK = 512, 768
FIRST_TILE = 256


def mm(a, b, cb=0):
    return lax.dot_general(a, b, (((1,), (cb,)), ((), ())), preferred_element_type=jnp.float32)


def normed(h):
    wide = h.astype(jnp.float32)
    scale = lax.rsqrt(jnp.mean(wide**2, -1, keepdims=True) + 1e-6)
    return wide, scale


def chunks(ff):
    return [pl.ds(i, CHUNK) for i in range(0, ff, CHUNK)]


def forward(h_ref, wg, wu, wd, next_ref, a_ref, p_ref, gate_ref, up_ref, between):
    wide, scale = normed(h_ref[...])
    a = (wide * scale).astype(jnp.bfloat16)
    a_ref[...] = a
    total = None
    for n, c in enumerate(chunks(wg.shape[-1])):
        between(n)
        gate, up = mm(a, wg[:, c]), mm(a, wu[:, c])
        gate_ref[:, c], up_ref[:, c] = gate, up
        p = (gate * jax.nn.sigmoid(gate) * up).astype(jnp.bfloat16)
        p_ref[:, c] = p
        part = mm(p, wd[c, :])
        total = part if total is None else total + part
    next_ref[...] = (wide + total.astype(jnp.bfloat16).astype(jnp.float32)).astype(jnp.bfloat16)


def gather_kernel(
    h_ref, gu_ref, d_ref, gu_out, d_out, next_ref, a_ref, p_ref, gate_ref, up_ref,
    wg, wu, wd, s1s, s1r, s2s, s2r, s3s, s3r, s4s, s4r, loc, load,
):
    step, steps = pl.program_id(0), pl.num_programs(0)
    x, me = lax.axis_index("rep"), lax.axis_index("dp")
    y, z, c = me // 8, (me // 2) % 4, me % 2
    rows, rows_d = gu_ref.shape[2], d_ref.shape[1]

    def at(yy, zz, cc):
        return (yy * Z + zz) * 2 + cc

    other = z + 1 - 2 * (z % 2)
    zs = [z, other, (z + 2) % 4, 3 - z]
    y_peer, c_peer, x_peer = (x, at(1 - y, z, c)), (x, at(y, z, 1 - c)), (1 - x, me)
    peers = [(x, at(y, zs[k], c)) for k in (1, 2, 3)] + [y_peer, c_peer, x_peer]

    groups = [(0, True), (0, False), (1, True), (1, False)]
    first, second, third = {}, {}, {}
    fourth = [[] for _ in groups]
    everything, locals_ = [], []

    def remote(src, dst, ss, rs, peer):
        copy = pltpu.make_async_remote_copy(src, dst, ss, rs, device_id=peer, device_id_type=MESH)
        everything.append(copy)
        return copy

    def own(l, gu, m):
        return gu_ref.at[m, l] if gu else d_ref.at[l]

    def place(l, gu, b, m):
        if gu:
            return gu_out.at[m, l, pl.ds(pl.multiple_of(b * rows, 8), rows)]
        return d_out.at[l, pl.ds(pl.multiple_of(b * rows_d, 16), rows_d)]

    def to_core(g, src, dst):
        n = len(fourth[g])
        copy = remote(src, dst, s4s.at[g, n], s4r.at[g, n], c_peer)
        fourth[g].append(copy)
        return copy

    begin, events = [], []
    for g, (l, gu) in enumerate(groups):
        for k in (1, 2, 3):
            peer = (x, at(y, zs[k], c))
            first[g, k] = remote(own(l, gu, x), place(l, gu, me, x), s1s.at[g, k - 1], s1r.at[g, k - 1], peer)
            begin.append(first[g, k])
    for g, (l, gu) in enumerate(groups):
        second[g, 0] = remote(own(l, gu, x), place(l, gu, me, x), s2s.at[g, 0], s2r.at[g, 0], y_peer)
        begin.append(second[g, 0])
        for m in (0, 1) if gu else (0,):
            src, dst = own(l, gu, m), place(l, gu, me, m)
            begin.append(to_core(g, src, dst))
            locals_.append(pltpu.make_async_copy(src, dst, loc.at[2 * g + m]))
            begin.append(locals_[-1])
    for g, (l, gu) in enumerate(groups):
        for k in (1, 2, 3):
            ref = place(l, gu, at(y, zs[k], c), x)
            second[g, k] = remote(ref, ref, s2s.at[g, k], s2r.at[g, k], y_peer)
            starts = [second[g, k]]
            if gu:
                third[g, k - 1] = remote(ref, ref, s3s.at[g // 2, k - 1], s3r.at[g // 2, k - 1], x_peer)
                starts.append(third[g, k - 1])
            events.append((4 * g + k + 1.0, l, first[g, k], starts + [to_core(g, ref, ref)]))
        for k in range(4):
            ref = place(l, gu, at(1 - y, zs[k], c), x)
            starts = []
            if gu:
                third[g, 3 + k] = remote(ref, ref, s3s.at[g // 2, 3 + k], s3r.at[g // 2, 3 + k], x_peer)
                starts.append(third[g, 3 + k])
            events.append((4 * g + k + 2.5, l, second[g, k], starts + [to_core(g, ref, ref)]))
        if gu:
            for j in range(7):
                b = at(y, zs[j + 1], c) if j < 3 else at(1 - y, zs[j - 3], c)
                ref = place(l, gu, b, 1 - x)
                events.append((7 * (g // 2) + j + 3.7, l, third[g, j], [to_core(g, ref, ref)]))
    events.sort(key=lambda e: (e[1], e[0]))

    def run(some):
        for _, _, arrival, starts in some:
            arrival.wait_recv()
            for copy in starts:
                copy.start()

    early = [e for e in events if e[1] == 0]
    late = [e for e in events if e[1] == 1]
    in_vmem = [
        pltpu.make_async_copy(src, dst, load.at[n])
        for n, (src, dst) in enumerate([(gu_out.at[0, 0], wg), (gu_out.at[1, 0], wu), (d_out.at[0], wd)])
    ]

    @pl.when(step == 0)
    def _():
        barrier = pltpu.get_barrier_semaphore()
        for peer in peers:
            pl.semaphore_signal(barrier, inc=1, device_id=peer, device_id_type=MESH)
        pl.semaphore_wait(barrier, len(peers))
        for copy in begin:
            copy.start()
        run(early)
        for copy in fourth[0] + fourth[1]:
            copy.wait_recv()
        for copy in locals_:
            copy.wait()
        for copy in in_vmem:
            copy.start()
        for copy in in_vmem:
            copy.wait()

    slots, done = {}, 0
    for n in range(1, TOKENS // FIRST_TILE):
        for part in range(3):
            slots[part, n] = [e for e in late[done:] if e[0] <= 10.3 + 0.9 * n + 0.3 * part]
            done += len(slots[part, n])

    def between(part):
        for (at_part, n), some in slots.items():
            if at_part == part and some:
                @pl.when(step == n)
                def _(some=some):
                    run(some)

    forward(h_ref, wg, wu, wd, next_ref, a_ref, p_ref, gate_ref, up_ref, between)

    @pl.when(step == steps - 1)
    def _():
        run(late[done:])
        for copy in fourth[2] + fourth[3]:
            copy.wait_recv()
        for copy in everything:
            copy.wait_send()


TOKENS = 2048


def gather(h, w_gate, w_up, w_down):
    gu = jnp.stack([w_gate, w_up])
    any_ = pl.BlockSpec(memory_space=pl.ANY)
    dma = pltpu.SemaphoreType.DMA
    _, layers, rows, ff = gu.shape
    _, rows_d, d = w_down.shape
    n, t, bf16, f32 = 16, h.shape[0], gu.dtype, jnp.float32
    outs = [(d, bf16), (d, bf16), (ff, bf16), (ff, f32), (ff, f32)]

    def tile(width):
        return pl.BlockSpec((FIRST_TILE, width), lambda i: (i, 0))

    return pl.pallas_call(
        gather_kernel,
        grid=(t // FIRST_TILE,),
        out_shape=[
            jax.ShapeDtypeStruct((2, layers, n * rows, ff), bf16),
            jax.ShapeDtypeStruct((layers, n * rows_d, d), bf16),
        ] + [jax.ShapeDtypeStruct((t, width), dtype) for width, dtype in outs],
        in_specs=[tile(d), any_, any_],
        out_specs=[any_, any_] + [tile(width) for width, _ in outs],
        scratch_shapes=[
            pltpu.VMEM((n * rows, ff), bf16), pltpu.VMEM((n * rows, ff), bf16), pltpu.VMEM((n * rows_d, d), bf16),
            dma((4, 3)), dma((4, 3)), dma((4, 4)), dma((4, 4)), dma((2, 7)), dma((2, 7)),
            dma((4, 16)), dma((4, 16)), dma((8,)), dma((3,)),
        ],
        compiler_params=pltpu.CompilerParams(
            collective_id=0, has_side_effects=True, vmem_limit_bytes=60 * 2**20, dimension_semantics=("arbitrary",)
        ),
    )(h, gu, w_down)


def through_gate(gate, up, dp):
    dp = dp.astype(jnp.bfloat16).astype(jnp.float32)
    s = jax.nn.sigmoid(gate)
    silu = gate * s
    dgate = (dp * up * (s * (1 + gate * (1 - s)))).astype(jnp.bfloat16)
    return silu, dgate, (dp * silu).astype(jnp.bfloat16)


def through_norm(wide, scale, dy, da_gate, da_up):
    bf16, f32 = jnp.bfloat16, jnp.float32
    da = (da_gate.astype(bf16).astype(f32) + da_up.astype(bf16).astype(f32)).astype(bf16).astype(f32)
    dh = scale * (da - wide * (scale**2 * jnp.mean(da * wide, -1, keepdims=True)))
    return (dy.astype(f32) + dh.astype(bf16).astype(f32)).astype(bf16)


def last_kernel(h_ref, dy_ref, wg, wu, wd, dh_ref, a_ref, p_ref, by_ref):
    wide, scale = normed(h_ref[...])
    a = (wide * scale).astype(jnp.bfloat16)
    a_ref[...] = a
    dy = dy_ref[...]
    da_gate = da_up = None
    for c in chunks(wg.shape[-1]):
        gate, up = mm(a, wg[:, c]), mm(a, wu[:, c])
        silu, dgate, dup = through_gate(gate, up, mm(dy, wd[c, :], 1))
        p_ref[:, c] = (silu * up).astype(jnp.bfloat16)
        by_ref[:, c], by_ref[:, pl.ds(wg.shape[-1] + c.start, CHUNK)] = dgate, dup
        g, u = mm(dgate, wg[:, c], 1), mm(dup, wu[:, c], 1)
        da_gate, da_up = (g, u) if da_gate is None else (da_gate + g, da_up + u)
    dh_ref[...] = through_norm(wide, scale, dy, da_gate, da_up)


def gate_kernel(dy_ref, gate_ref, up_ref, wd, dgate_ref, dup_ref):
    dy = dy_ref[...]
    for c in chunks(gate_ref.shape[-1]):
        _, dgate_ref[:, c], dup_ref[:, c] = through_gate(gate_ref[:, c], up_ref[:, c], mm(dy, wd[c, :], 1))


def input_kernel(h_ref, dy_ref, dgate_ref, dup_ref, wg, wu, dh_ref):
    wide, scale = normed(h_ref[...])
    da_gate, da_up = mm(dgate_ref[...], wg[...], 1), mm(dup_ref[...], wu[...], 1)
    dh_ref[...] = through_norm(wide, scale, dy_ref[...], da_gate, da_up)


def call(kernel, tokens, weights, outs, matmuls, t=None, part=0, tile=TILE):
    t = t or tokens[0].shape[0]
    d, ff, skip = 896, 2304, part * t // tile
    specs = [pl.BlockSpec((tile, v.shape[1]), lambda i: (i + skip, 0)) for v in tokens]
    for w, at in weights:
        specs.append(
            pl.BlockSpec((None,) * len(at) + w.shape[-2:], lambda i, at=at: (*at, 0, 0), pipeline_mode=pl.Buffered(1))
        )
    return pl.pallas_call(
        kernel,
        grid=(t // tile,),
        in_specs=specs,
        out_specs=[pl.BlockSpec((tile, n), lambda i: (i, 0)) for n, _ in outs],
        out_shape=[jax.ShapeDtypeStruct((t, n), dtype) for n, dtype in outs],
        compiler_params=pltpu.CompilerParams(vmem_limit_bytes=60 * 2**20, dimension_semantics=("arbitrary",)),
        cost_estimate=pl.CostEstimate(flops=2 * t * d * ff * matmuls, bytes_accessed=30 * 2**20, transcendentals=t * ff),
    )(*tokens, *(w for w, _ in weights))


def dot(a, b, ca, cb):
    return lax.dot_general(a, b, (((ca,), (cb,)), ((), ())), preferred_element_type=jnp.float32)


def pairs(of):
    return [((y * Z + z) * 2 + c, of(y, z, c)) for y in range(2) for z in range(Z) for c in range(2)]


def scatter_sum(term):
    me = lax.axis_index("dp")
    y, z, c = me // 8, (me // 2) % 4, me % 2
    term = lax.optimization_barrier(term).reshape(2, Z, 2, -1, term.shape[-1])

    def pick(t, i, axis):
        return lax.dynamic_index_in_dim(t, i, axis, keepdims=False)

    def swap(t, of):
        t = t.astype(jnp.bfloat16)
        t = lax.ppermute(t, "dp", pairs(of))
        return t.astype(jnp.float32)

    got = swap(pick(term, 1 - c, 2), lambda y, z, c: (y * Z + z) * 2 + 1 - c)
    term = pick(term, c, 2) + got
    got = swap(pick(term, 1 - y, 0), lambda y, z, c: ((1 - y) * Z + z) * 2 + c)
    term = pick(term, y, 0) + got
    total = pick(term, z, 0)
    for k in (1, 2, 3):
        total += swap(pick(term, z ^ k, 0), lambda y, z, c: (y * Z + (z ^ k)) * 2 + c)
    return total.astype(jnp.bfloat16)


def solution(mesh):
    def step(*args):
        return work(*args)

    def work(x, dy, w_gate, w_up, w_down):
        x, dy = x[0], dy[0]
        bf16 = jnp.bfloat16
        gu, down, h, a0, p0, gate, up = gather(x, w_gate, w_up, w_down)
        d, ff = x.shape[1], gu.shape[-1]
        wg, wu, wd = [[(gu, (0, l)) for l in (0, 1)], [(gu, (1, l)) for l in (0, 1)], [(down, (l,)) for l in (0, 1)]]
        dy0, a1, p1, by1 = call(
            last_kernel, (h, dy), (wg[1], wu[1], wd[1]), [(d, bf16), (d, bf16), (ff, bf16), (2 * ff, bf16)], 5
        )
        d1 = scatter_sum(dot(p1, dy, 0, 0))
        gu1 = scatter_sum(dot(a1, by1, 0, 0))
        g1, u1 = gu1[:, :ff], gu1[:, ff:]
        d0 = scatter_sum(dot(p0, dy0, 0, 0))
        dgate0, dup0 = call(gate_kernel, (dy0, gate, up), (wd[0],), [(ff, bf16), (ff, bf16)], 1, tile=256)
        g0 = scatter_sum(dot(a0, dgate0, 0, 0))
        u0 = scatter_sum(dot(a0, dup0, 0, 0))
        half = x.shape[0] // 2
        dx = jnp.concatenate([
            call(input_kernel, (x, dy0, dgate0, dup0), (wg[0], wu[0]), [(d, bf16)], 1, half, n)[0]
            for n in (0, 1)
        ])
        return dx[None], jnp.stack([g0, g1]), jnp.stack([u0, u1]), jnp.stack([d0, d1])

    rows = P(("rep", "dp"), None, None)
    w = P(None, "dp", None)
    g = P("rep", "dp", None)
    step = jax.shard_map(step, mesh=mesh, in_specs=(rows, rows, w, w, w), out_specs=(rows, g, g, g), check_vma=False)
    return step
```

```python
import jax
import jax.numpy as jnp
from jax import lax
from jax.experimental import pallas as pl
from jax.experimental.pallas import tpu as pltpu
from jax.sharding import PartitionSpec as P


MESH = pl.DeviceIdType.MESH
Z = 4


TILE, CHUNK = 512, 768
FIRST_TILE = 256


def mm(a, b, cb=0):
    return lax.dot_general(a, b, (((1,), (cb,)), ((), ())), preferred_element_type=jnp.float32)


def normed(h):
    wide = h.astype(jnp.float32)
    scale = lax.rsqrt(jnp.mean(wide**2, -1, keepdims=True) + 1e-6)
    return wide, scale


def chunks(ff):
    return [pl.ds(i, CHUNK) for i in range(0, ff, CHUNK)]


def forward(h_ref, wg, wu, wd, next_ref, a_ref, p_ref, gate_ref, up_ref):
    wide, scale = normed(h_ref[...])
    a = (wide * scale).astype(jnp.bfloat16)
    a_ref[...] = a
    total = None
    for c in chunks(wg.shape[-1]):
        gate, up = mm(a, wg[:, c]), mm(a, wu[:, c])
        gate_ref[:, c], up_ref[:, c] = gate, up
        p = (gate * jax.nn.sigmoid(gate) * up).astype(jnp.bfloat16)
        p_ref[:, c] = p
        part = mm(p, wd[c, :])
        total = part if total is None else total + part
    next_ref[...] = (wide + total.astype(jnp.bfloat16).astype(jnp.float32)).astype(jnp.bfloat16)


def gather_kernel(
    h_ref, gu_ref, d_ref, gu_out, d_out, next_ref, a_ref, p_ref, gate_ref, up_ref,
    wg, wu, wd, s1s, s1r, s2s, s2r, s3s, s3r, s4s, s4r, loc, load,
):
    step, steps = pl.program_id(0), pl.num_programs(0)
    x, me = lax.axis_index("rep"), lax.axis_index("dp")
    y, z, c = me // 8, (me // 2) % 4, me % 2
    rows, rows_d = gu_ref.shape[2], d_ref.shape[1]

    def at(yy, zz, cc):
        return (yy * Z + zz) * 2 + cc

    other = z + 1 - 2 * (z % 2)
    zs = [z, other, (z + 2) % 4, 3 - z]
    y_peer, c_peer, x_peer = (x, at(1 - y, z, c)), (x, at(y, z, 1 - c)), (1 - x, me)
    peers = [(x, at(y, zs[k], c)) for k in (1, 2, 3)] + [y_peer, c_peer, x_peer]

    groups = [(0, True), (0, False), (1, True), (1, False)]
    first, second, third = {}, {}, {}
    fourth = [[] for _ in groups]
    everything, locals_ = [], []

    def remote(src, dst, ss, rs, peer):
        copy = pltpu.make_async_remote_copy(src, dst, ss, rs, device_id=peer, device_id_type=MESH)
        everything.append(copy)
        return copy

    def own(l, gu, m):
        return gu_ref.at[m, l] if gu else d_ref.at[l]

    def place(l, gu, b, m):
        if gu:
            return gu_out.at[m, l, pl.ds(pl.multiple_of(b * rows, 8), rows)]
        return d_out.at[l, pl.ds(pl.multiple_of(b * rows_d, 16), rows_d)]

    def to_core(g, src, dst):
        n = len(fourth[g])
        copy = remote(src, dst, s4s.at[g, n], s4r.at[g, n], c_peer)
        fourth[g].append(copy)
        return copy

    begin, events = ([], []), []
    for g, (l, gu) in enumerate(groups):
        for k in (1, 2, 3):
            peer = (x, at(y, zs[k], c))
            first[g, k] = remote(own(l, gu, x), place(l, gu, me, x), s1s.at[g, k - 1], s1r.at[g, k - 1], peer)
            begin[l].append(first[g, k])
    for g, (l, gu) in enumerate(groups):
        second[g, 0] = remote(own(l, gu, x), place(l, gu, me, x), s2s.at[g, 0], s2r.at[g, 0], y_peer)
        begin[l].append(second[g, 0])
        for m in (0, 1) if gu else (0,):
            src, dst = own(l, gu, m), place(l, gu, me, m)
            begin[l].append(to_core(g, src, dst))
            locals_.append(pltpu.make_async_copy(src, dst, loc.at[2 * g + m]))
            begin[l].append(locals_[-1])
    for g, (l, gu) in enumerate(groups):
        for k in (1, 2, 3):
            ref = place(l, gu, at(y, zs[k], c), x)
            second[g, k] = remote(ref, ref, s2s.at[g, k], s2r.at[g, k], y_peer)
            starts = [second[g, k]]
            if gu:
                third[g, k - 1] = remote(ref, ref, s3s.at[g // 2, k - 1], s3r.at[g // 2, k - 1], x_peer)
                starts.append(third[g, k - 1])
            starts.append(to_core(g, ref, ref))
            events.append((4 * g + k + 1.0, l, first[g, k], starts + (begin[1] if (g, k) == (1, 3) else [])))
        for k in range(4):
            ref = place(l, gu, at(1 - y, zs[k], c), x)
            starts = []
            if gu:
                third[g, 3 + k] = remote(ref, ref, s3s.at[g // 2, 3 + k], s3r.at[g // 2, 3 + k], x_peer)
                starts.append(third[g, 3 + k])
            events.append((4 * g + k + 2.5, l, second[g, k], starts + [to_core(g, ref, ref)]))
        if gu:
            for j in range(7):
                b = at(y, zs[j + 1], c) if j < 3 else at(1 - y, zs[j - 3], c)
                ref = place(l, gu, b, 1 - x)
                events.append((7 * (g // 2) + j + 3.7, l, third[g, j], [to_core(g, ref, ref)]))
    events.sort(key=lambda e: (e[1], e[0]))

    def run(some):
        for _, _, arrival, starts in some:
            arrival.wait_recv()
            for copy in starts:
                copy.start()

    early = [e for e in events if e[1] == 0]
    late = [e for e in events if e[1] == 1]
    in_vmem = [
        pltpu.make_async_copy(src, dst, load.at[n])
        for n, (src, dst) in enumerate([(gu_out.at[0, 0], wg), (gu_out.at[1, 0], wu), (d_out.at[0], wd)])
    ]

    @pl.when(step == 0)
    def _():
        barrier = pltpu.get_barrier_semaphore()
        for peer in peers:
            pl.semaphore_signal(barrier, inc=1, device_id=peer, device_id_type=MESH)
        pl.semaphore_wait(barrier, len(peers))
        for copy in begin[0]:
            copy.start()
        run(early)
        for copy in fourth[0] + fourth[1]:
            copy.wait_recv()
        for copy in locals_:
            copy.wait()
        for copy in in_vmem:
            copy.start()
        for copy in in_vmem:
            copy.wait()

    done = 0
    for n in range(1, TOKENS // FIRST_TILE):
        some = [e for e in late[done:] if e[0] <= 10.5 + 0.9 * n]
        done += len(some)
        if some:
            @pl.when(step == n)
            def _(some=some):
                run(some)

    forward(h_ref, wg, wu, wd, next_ref, a_ref, p_ref, gate_ref, up_ref)

    @pl.when(step == steps - 1)
    def _():
        run(late[done:])
        for copy in fourth[2] + fourth[3]:
            copy.wait_recv()
        for copy in everything:
            copy.wait_send()


TOKENS = 2048


def gather(h, w_gate, w_up, w_down):
    gu = jnp.stack([w_gate, w_up])
    any_ = pl.BlockSpec(memory_space=pl.ANY)
    dma = pltpu.SemaphoreType.DMA
    _, layers, rows, ff = gu.shape
    _, rows_d, d = w_down.shape
    n, t, bf16, f32 = 16, h.shape[0], gu.dtype, jnp.float32
    outs = [(d, bf16), (d, bf16), (ff, bf16), (ff, f32), (ff, f32)]

    def tile(width):
        return pl.BlockSpec((FIRST_TILE, width), lambda i: (i, 0))

    return pl.pallas_call(
        gather_kernel,
        grid=(t // FIRST_TILE,),
        out_shape=[
            jax.ShapeDtypeStruct((2, layers, n * rows, ff), bf16),
            jax.ShapeDtypeStruct((layers, n * rows_d, d), bf16),
        ] + [jax.ShapeDtypeStruct((t, width), dtype) for width, dtype in outs],
        in_specs=[tile(d), any_, any_],
        out_specs=[any_, any_] + [tile(width) for width, _ in outs],
        scratch_shapes=[
            pltpu.VMEM((n * rows, ff), bf16), pltpu.VMEM((n * rows, ff), bf16), pltpu.VMEM((n * rows_d, d), bf16),
            dma((4, 3)), dma((4, 3)), dma((4, 4)), dma((4, 4)), dma((2, 7)), dma((2, 7)),
            dma((4, 16)), dma((4, 16)), dma((8,)), dma((3,)),
        ],
        compiler_params=pltpu.CompilerParams(
            collective_id=0, has_side_effects=True, vmem_limit_bytes=60 * 2**20, dimension_semantics=("arbitrary",)
        ),
    )(h, gu, w_down)


def through_gate(gate, up, dp):
    dp = dp.astype(jnp.bfloat16).astype(jnp.float32)
    s = jax.nn.sigmoid(gate)
    silu = gate * s
    dgate = (dp * up * (s * (1 + gate * (1 - s)))).astype(jnp.bfloat16)
    return silu, dgate, (dp * silu).astype(jnp.bfloat16)


def through_norm(wide, scale, dy, da_gate, da_up):
    bf16, f32 = jnp.bfloat16, jnp.float32
    da = (da_gate.astype(bf16).astype(f32) + da_up.astype(bf16).astype(f32)).astype(bf16).astype(f32)
    dh = scale * (da - wide * (scale**2 * jnp.mean(da * wide, -1, keepdims=True)))
    return (dy.astype(f32) + dh.astype(bf16).astype(f32)).astype(bf16)


def last_kernel(h_ref, dy_ref, wg, wu, wd, dh_ref, a_ref, p_ref, by_ref):
    wide, scale = normed(h_ref[...])
    a = (wide * scale).astype(jnp.bfloat16)
    a_ref[...] = a
    dy = dy_ref[...]
    da_gate = da_up = None
    for c in chunks(wg.shape[-1]):
        gate, up = mm(a, wg[:, c]), mm(a, wu[:, c])
        silu, dgate, dup = through_gate(gate, up, mm(dy, wd[c, :], 1))
        p_ref[:, c] = (silu * up).astype(jnp.bfloat16)
        by_ref[:, c], by_ref[:, pl.ds(wg.shape[-1] + c.start, CHUNK)] = dgate, dup
        g, u = mm(dgate, wg[:, c], 1), mm(dup, wu[:, c], 1)
        da_gate, da_up = (g, u) if da_gate is None else (da_gate + g, da_up + u)
    dh_ref[...] = through_norm(wide, scale, dy, da_gate, da_up)


def gate_kernel(dy_ref, gate_ref, up_ref, wd, dgate_ref, dup_ref):
    dy = dy_ref[...]
    for c in chunks(gate_ref.shape[-1]):
        _, dgate_ref[:, c], dup_ref[:, c] = through_gate(gate_ref[:, c], up_ref[:, c], mm(dy, wd[c, :], 1))


def input_kernel(h_ref, dy_ref, dgate_ref, dup_ref, wg, wu, dh_ref):
    wide, scale = normed(h_ref[...])
    da_gate, da_up = mm(dgate_ref[...], wg[...], 1), mm(dup_ref[...], wu[...], 1)
    dh_ref[...] = through_norm(wide, scale, dy_ref[...], da_gate, da_up)


def call(kernel, tokens, weights, outs, matmuls, t=None, part=0, tile=TILE, into=None):
    t = t or tokens[0].shape[0]
    d, ff, skip = 896, 2304, part * t // tile
    specs = [pl.BlockSpec((tile, v.shape[1]), lambda i: (i + skip, 0)) for v in tokens]
    for w, at in weights:
        specs.append(
            pl.BlockSpec((None,) * len(at) + w.shape[-2:], lambda i, at=at: (*at, 0, 0), pipeline_mode=pl.Buffered(1))
        )
    more, alias = [], {}
    if into is not None:
        specs.append(pl.BlockSpec(memory_space=pl.ANY))
        more, alias, inner = [into], {len(tokens) + len(weights): 0}, kernel

        def kernel(*refs):
            inner(*refs[: -len(outs) - 1], *refs[-len(outs) :])

    return pl.pallas_call(
        kernel,
        grid=(t // tile,),
        in_specs=specs,
        out_specs=[pl.BlockSpec((tile, n), lambda i: (i + skip, 0)) for n, _ in outs],
        input_output_aliases=alias,
        out_shape=[jax.ShapeDtypeStruct((tokens[0].shape[0], n), dtype) for n, dtype in outs],
        compiler_params=pltpu.CompilerParams(vmem_limit_bytes=60 * 2**20, dimension_semantics=("arbitrary",)),
        cost_estimate=pl.CostEstimate(flops=2 * t * d * ff * matmuls, bytes_accessed=30 * 2**20, transcendentals=t * ff),
    )(*tokens, *(w for w, _ in weights), *more)


def dot(a, b, ca, cb):
    return lax.dot_general(a, b, (((ca,), (cb,)), ((), ())), preferred_element_type=jnp.float32)


def pairs(of):
    return [((y * Z + z) * 2 + c, of(y, z, c)) for y in range(2) for z in range(Z) for c in range(2)]


def scatter_sum(term):
    me = lax.axis_index("dp")
    y, z, c = me // 8, (me // 2) % 4, me % 2
    term = lax.optimization_barrier(term).reshape(2, Z, 2, -1, term.shape[-1])

    def pick(t, i, axis):
        return lax.dynamic_index_in_dim(t, i, axis, keepdims=False)

    def swap(t, of):
        t = t.astype(jnp.bfloat16)
        t = lax.ppermute(t, "dp", pairs(of))
        return t.astype(jnp.float32)

    got = swap(pick(term, 1 - c, 2), lambda y, z, c: (y * Z + z) * 2 + 1 - c)
    term = pick(term, c, 2) + got
    got = swap(pick(term, 1 - y, 0), lambda y, z, c: ((1 - y) * Z + z) * 2 + c)
    term = pick(term, y, 0) + got
    total = pick(term, z, 0)
    for k in (1, 2, 3):
        total += swap(pick(term, z ^ k, 0), lambda y, z, c: (y * Z + (z ^ k)) * 2 + c)
    return total.astype(jnp.bfloat16)


def solution(mesh):
    def step(*args):
        return work(*args)

    def work(x, dy, w_gate, w_up, w_down):
        x, dy = x[0], dy[0]
        bf16 = jnp.bfloat16
        gu, down, h, a0, p0, gate, up = gather(x, w_gate, w_up, w_down)
        d, ff = x.shape[1], gu.shape[-1]
        wg, wu, wd = [[(gu, (0, l)) for l in (0, 1)], [(gu, (1, l)) for l in (0, 1)], [(down, (l,)) for l in (0, 1)]]
        dy0, a1, p1, by1 = call(
            last_kernel, (h, dy), (wg[1], wu[1], wd[1]), [(d, bf16), (d, bf16), (ff, bf16), (2 * ff, bf16)], 5
        )
        d1 = scatter_sum(dot(p1, dy, 0, 0))
        gu1 = scatter_sum(dot(a1, by1, 0, 0))
        g1, u1 = gu1[:, :ff], gu1[:, ff:]
        d0 = scatter_sum(dot(p0, dy0, 0, 0))
        dgate0, dup0 = call(gate_kernel, (dy0, gate, up), (wd[0],), [(ff, bf16), (ff, bf16)], 1, tile=256)
        g0 = scatter_sum(dot(a0, dgate0, 0, 0))
        u0 = scatter_sum(dot(a0, dup0, 0, 0))
        half, dx = x.shape[0] // 2, None
        for n in (0, 1):
            (dx,) = call(input_kernel, (x, dy0, dgate0, dup0), (wg[0], wu[0]), [(d, bf16)], 1, half, n, into=dx)
        return dx[None], jnp.stack([g0, g1]), jnp.stack([u0, u1]), jnp.stack([d0, d1])

    rows = P(("rep", "dp"), None, None)
    w = P(None, "dp", None)
    g = P("rep", "dp", None)
    step = jax.shard_map(step, mesh=mesh, in_specs=(rows, rows, w, w, w), out_specs=(rows, g, g, g), check_vma=False)
    return step
```
